32 devices in a mesh: vocab: 8 (over z, y), batch: 4 (over x, core).
Axes of the slice: x: 2, y: 2, z: 4, core: 2. Of those that a mesh axis runs over, the one named last changes fastest.
Arguments:
- latent_state_rows: bfloat16 [64, 8192], P('batch', 'vocab'), may hold values from -90 to 90
- closing_rescale_coeffs: bfloat16 [8192], replicated, may hold values from 0.5 to 1.5
- output_projection_matrix: bfloat16 [8192, 131072], P(None, ('vocab', 'batch')), may hold values from -3.7565048 to 3.7565048
- config_heat_values: float32 [16], replicated, may hold values from 0.7 to 1.4
- sequence_config_choice: int32 [64], replicated, may hold values from 0 to 15
- ranked_choice_ids: int32 [64, 128], replicated, may hold values from 0 to 131071
- keep_count: int32 [64], replicated, may hold values from 2 to 128
Outputs:
- log_norm: float32 [64], P('batch')
- kept_mass: float32 [64], P('batch')
- renormed: float32 [64, 128], P('batch')
The draws below stay inside these ranges and needn't reach their ends.
All inputs are finite; a program needn't handle non-finite values.
Results may differ from the reference program's by a relative error of at most 0.0048.
Values may be sent and summed in bfloat16 or wider, within the bound.
A program may use at most 128 MiB of HBM per device.

```python
import math
import jax
import jax.numpy as jnp
from jax import lax

D = 8192
VOCAB = 131072
CAND = 128
SAMPLER_CONFIGS = 16
SG = 16
SLOTS = 64
N_VOCAB = 8
N_BATCH = 4


def weight_block(key, block):
    return jnp.clip(jax.random.normal(jax.random.fold_in(jax.random.fold_in(key, 11), block), (D, 128), jnp.float32), -5.0, 5.0)


def column_scale(key):
    position = jnp.arange(VOCAB, dtype=jnp.float32) / VOCAB
    spread = jnp.exp(jax.random.uniform(jax.random.fold_in(key, 12), (VOCAB,), jnp.float32, math.log(0.45), math.log(2.2)))
    trend = 0.75 + 0.5 * position
    return 2.0 * spread * trend


def drawn_pairs():
    pairs = []
    targets = [160.0, 200.0, 240.0, 160.0, 200.0, 240.0]
    for number in range(6):
        first_id = (5003 + 24011 * number) % VOCAB
        second_id = (first_id + 7) % VOCAB
        row_index = number * SLOTS // 6
        pairs.append((first_id, second_id, row_index, targets[number]))
    return pairs


def draw_output_projection_matrix(key, part):
    blocks = jax.vmap(lambda block: weight_block(key, block), out_axes=1)(jnp.arange(VOCAB // 128))
    matrix = blocks.reshape(D, VOCAB) * (column_scale(key) / math.sqrt(D))[None, :]
    return matrix.astype(jnp.bfloat16)


def draw_latent_state_rows(key, part):
    values = jnp.clip(jax.random.normal(jax.random.fold_in(key, 13), (SLOTS, D), jnp.float32), -5.0, 5.0)
    return values.astype(jnp.bfloat16)


def draw_ranked_choice_ids(key, part):
    ids = jax.random.randint(jax.random.fold_in(key, 16), (SLOTS, CAND), 0, VOCAB, jnp.int32)
    shard_count = N_VOCAB * N_BATCH
    shard_width = VOCAB // shard_count
    group_of = jnp.arange(SLOTS, dtype=jnp.int32) // SG
    offsets = jax.random.randint(jax.random.fold_in(key, 17), (SLOTS, 2), 0, shard_width, jnp.int32)
    near_shard = (group_of + 1) % shard_count
    far_shard = (group_of + shard_count // 2) % shard_count
    ids = ids.at[:, 0].set(near_shard * shard_width + offsets[:, 0])
    ids = ids.at[:, 1].set(far_shard * shard_width + offsets[:, 1])
    for first_id, second_id, row_index, target in drawn_pairs():
        ids = ids.at[row_index, 0].set(jnp.int32(first_id))
        ids = ids.at[row_index, 1].set(jnp.int32(second_id))
    return ids


def touch_ends(values, own_key, low, top_value):
    extent = values.shape
    place = [jax.random.randint(jax.random.fold_in(own_key, axis), (), 0, extent[axis]) for axis in range(len(extent))]
    values = values.at[tuple(place)].set(low)
    longest = extent.index(max(extent))
    place[longest] = (place[longest] + 1) % extent[longest]
    return values.at[tuple(place)].set(top_value)


def setup_inputs(seed: int = 0) -> dict:
    key_list = jax.random.split(jax.random.key(seed), 8)
    latent_state_rows = draw_latent_state_rows(jax.random.fold_in(key_list[7], 71), 0)
    closing_rescale_coeffs = jnp.clip(1.0 + 0.1 * jax.random.normal(key_list[1], (D,), jnp.float32), 0.5, 1.5).astype(jnp.bfloat16)
    output_projection_matrix = draw_output_projection_matrix(jax.random.fold_in(key_list[7], 71), 0)
    config_heat_values = jnp.clip(jnp.exp(jax.random.uniform(key_list[3], (SAMPLER_CONFIGS,), jnp.float32, math.log(0.7), math.log(1.4))), 0.7, 1.4)
    sequence_config_choice = touch_ends(jax.random.randint(key_list[4], (SLOTS,), 0, SAMPLER_CONFIGS), jax.random.fold_in(key_list[4], 1), 0, SAMPLER_CONFIGS - 1).astype(jnp.int32)
    ranked_choice_ids = draw_ranked_choice_ids(jax.random.fold_in(key_list[7], 71), 0)
    keep_count = touch_ends(jax.random.randint(key_list[6], (SLOTS,), 2, CAND + 1), jax.random.fold_in(key_list[6], 1), 2, CAND).astype(jnp.int32)
    return {"latent_state_rows": latent_state_rows, "closing_rescale_coeffs": closing_rescale_coeffs, "output_projection_matrix": output_projection_matrix, "config_heat_values": config_heat_values, "sequence_config_choice": sequence_config_choice, "ranked_choice_ids": ranked_choice_ids, "keep_count": keep_count}


epsilon = 1e-06

def reference(latent_state_rows, closing_rescale_coeffs, output_projection_matrix, config_heat_values, sequence_config_choice, ranked_choice_ids, keep_count):
    values = latent_state_rows.astype(jnp.float32)
    mean_square = lax.optimization_barrier(jnp.mean(values * values, axis=1, keepdims=True))
    normed = (values * lax.rsqrt(mean_square + epsilon) * closing_rescale_coeffs.astype(jnp.float32)[None, :]).astype(jnp.bfloat16)
    unnormalized_scores = jnp.dot(normed, output_projection_matrix, preferred_element_type=jnp.float32)
    config_membership = (sequence_config_choice[:, None] == jnp.arange(SAMPLER_CONFIGS, dtype=jnp.int32)[None, :]).astype(jnp.float32)
    sequence_heat_values = lax.optimization_barrier(jnp.sum(config_membership * config_heat_values[None, :], axis=1))
    divided_scores = unnormalized_scores / sequence_heat_values[:, None]
    row_top = lax.optimization_barrier(jnp.max(divided_scores, axis=1))
    row_total = lax.optimization_barrier(jnp.sum(jnp.exp(divided_scores - row_top[:, None]), axis=1))
    log_norm = row_top + jnp.log(row_total)
    picked = jnp.take_along_axis(divided_scores, ranked_choice_ids.astype(jnp.int32), axis=1)
    kept_mask = jnp.arange(CAND, dtype=jnp.int32)[None, :] < keep_count[:, None]
    kept_top = lax.optimization_barrier(jnp.max(jnp.where(kept_mask, picked, jnp.float32(-3e+38)), axis=1))
    shifted = jnp.where(kept_mask, picked - kept_top[:, None], jnp.float32(0.0))
    kept_exp = jnp.where(kept_mask, jnp.exp(shifted), jnp.float32(0.0))
    kept_sum = lax.optimization_barrier(jnp.sum(kept_exp, axis=1))
    kept_mass = kept_top + jnp.log(kept_sum) - log_norm
    return (log_norm, kept_mass, kept_exp / kept_sum[:, None])
```

```python
import functools

import jax
import jax.numpy as jnp
from jax import lax
from jax.experimental import pallas as pl
from jax.experimental.pallas import tpu as pltpu
from jax.sharding import PartitionSpec as P

MESH = pl.DeviceIdType.MESH
epsilon = 1e-06
LANES = 128
STAT_ROWS = 8
CHUNK_ROWS = 512
STREAM_BYTES = 48 * 1024 * 1024


def iota(shape, axis):
    return lax.broadcasted_iota(jnp.int32, shape, axis)


def column_to_row(column):
    rows = column.shape[0]
    diagonal = iota((rows, LANES), 0) == iota((rows, LANES), 1)
    return jnp.sum(jnp.where(diagonal, column, 0.0), axis=0, keepdims=True)


def row_to_column(row, first, rows):
    width = row.shape[1]
    diagonal = iota((rows, width), 0) + first == iota((rows, width), 1)
    return jnp.sum(jnp.where(diagonal, row, 0.0), axis=1, keepdims=True)


def combine(parts, group):
    candidates = parts[0][:group, :]
    top = parts[0][group : group + 1, :]
    for part in parts[1:]:
        candidates = candidates + part[:group, :]
        top = jnp.maximum(top, part[group : group + 1, :])
    total = jnp.zeros_like(top)
    for part in parts:
        total = total + part[group + 1 : group + 2, :] * jnp.exp(
            part[group : group + 1, :] - top
        )
    return candidates, top, total


def kernel(
    n_v,
    n_b,
    n_slots,
    kc,
    x_ref,
    gain_ref,
    w_ref,
    heat_ref,
    choice_ref,
    ids_ref,
    keep_ref,
    norm_ref,
    mass_ref,
    renorm_ref,
    wbuf,
    xbuf,
    lhs,
    acc,
    outbox,
    inbox,
    midbox,
    lastbox,
    w_sem,
    x_recv,
    a_send,
    x_send,
    c_send,
    t_send,
    t_recv,
    u_send,
    u_recv,
):
    v = lax.axis_index("vocab")
    b = lax.axis_index("batch")
    n_x = n_b // 2
    x = b // 2
    c = b % 2
    partner = 2 * x + (1 - c)
    group, fpd = x_ref.shape
    slots = n_b * group
    depth, cols = w_ref.shape
    n_k = depth // kc
    per_block = fpd // kc

    def stream(k):
        slot = lax.rem(k, n_slots)
        return pltpu.make_async_copy(
            w_ref.at[pl.ds(pl.multiple_of(k * kc, kc), kc), :], wbuf.at[slot], w_sem.at[slot]
        )

    for k in range(n_slots):
        stream(k).start()

    barrier = pltpu.get_barrier_semaphore()
    for j in range(1, n_v):
        pl.semaphore_signal(barrier, inc=1, device_id=((v + j) % n_v, b), device_id_type=MESH)
    for j in range(1, n_b):
        pl.semaphore_signal(barrier, inc=1, device_id=(v, (b + j) % n_b), device_id_type=MESH)
    pl.semaphore_wait(barrier, n_v - 1 + n_b - 1)

    def send(src, dst, send_sem, recv_sem, to):
        copy = pltpu.make_async_remote_copy(
            src_ref=src,
            dst_ref=dst,
            send_sem=send_sem,
            recv_sem=recv_sem,
            device_id=to,
            device_id_type=MESH,
        )
        copy.start()
        return copy

    def arrived(row, col):
        pltpu.make_async_copy(x_ref, xbuf.at[row, col], x_recv.at[row, col]).wait()

    sent = []
    for j in range(1, n_v):
        sent.append(
            send(x_ref, xbuf.at[b, v], a_send.at[j], x_recv.at[b, v], ((v + j) % n_v, b))
        )
    for j in range(n_v):
        origin = (v - j + n_v) % n_v
        block = x_ref if j == 0 else xbuf.at[b, origin]
        if j > 0:
            arrived(b, origin)
        for i in range(1, n_x):
            to = 2 * ((x + i) % n_x) + c
            sent.append(
                send(block, xbuf.at[b, origin], x_send.at[i, j], x_recv.at[b, origin], (v, to))
            )
        sent.append(
            send(block, xbuf.at[b, origin], c_send.at[0, j], x_recv.at[b, origin], (v, partner))
        )
    for j in range(n_v):
        for i in range(1, n_x):
            origin = (v - j + n_v) % n_v
            source = 2 * ((x - i + n_x) % n_x) + c
            arrived(source, origin)
            block = xbuf.at[source, origin]
            sent.append(
                send(block, block, c_send.at[i, j], x_recv.at[source, origin], (v, partner))
            )
    for j in range(n_v):
        for i in range(n_x):
            origin = (v - j + n_v) % n_v
            source = 2 * ((x - i + n_x) % n_x) + (1 - c)
            arrived(source, origin)
    xbuf[b, v] = x_ref[...]

    def square(f, carry):
        values = xbuf[:, f].reshape(slots, fpd).astype(jnp.float32)
        values = values * values
        for t in range(fpd // LANES):
            carry = carry + values[:, t * LANES : (t + 1) * LANES]
        return carry

    squares = lax.fori_loop(0, n_v, square, jnp.zeros((slots, LANES), jnp.float32))
    mean_square = jnp.sum(squares, axis=1, keepdims=True) / depth
    factor = lax.rsqrt(mean_square + epsilon)

    def rescale(f, carry):
        values = xbuf[:, f].reshape(slots, fpd).astype(jnp.float32)
        gain = gain_ref[pl.ds(f, 1), :]
        normed = (values * factor * gain).astype(jnp.bfloat16)
        for i in range(per_block):
            lhs[f * per_block + i] = normed[:, i * kc : (i + 1) * kc]
        return carry

    lax.fori_loop(0, n_v, rescale, 0)

    acc[...] = jnp.zeros_like(acc)

    def multiply(k, carry):
        slot = lax.rem(k, n_slots)
        stream(k).wait()
        acc[...] += jnp.dot(lhs[k], wbuf[slot], preferred_element_type=jnp.float32)

        @pl.when(k + n_slots < n_k)
        def _():
            stream(k + n_slots).start()

        return carry

    lax.fori_loop(0, n_k, multiply, 0)

    choice = row_to_column(choice_ref[...].astype(jnp.float32), 0, slots)
    n_heat = heat_ref.shape[1]
    member = choice == iota((slots, n_heat), 1).astype(jnp.float32)
    heat = jnp.sum(jnp.where(member, heat_ref[...], 0.0), axis=1, keepdims=True)

    local_ids = ids_ref[...] - (v * n_b + b) * cols
    tile_of = local_ids >> 7
    lane_of = local_ids & (LANES - 1)
    picked = jnp.zeros((slots, LANES), jnp.float32)
    top = jnp.full((slots, LANES), -3e38, jnp.float32)
    for t in range(cols // LANES):
        part = acc[:, t * LANES : (t + 1) * LANES] / heat
        acc[:, t * LANES : (t + 1) * LANES] = part
        top = jnp.maximum(top, part)
        found = jnp.take_along_axis(part, lane_of, axis=1, mode="promise_in_bounds")
        picked = jnp.where(tile_of == t, found, picked)
    top = jnp.max(top, axis=1, keepdims=True)
    total = jnp.zeros((slots, LANES), jnp.float32)
    for t in range(cols // LANES):
        total = total + jnp.exp(acc[:, t * LANES : (t + 1) * LANES] - top)
    total = jnp.sum(total, axis=1, keepdims=True)

    for p in range(n_b):
        rows = slice(p * group, (p + 1) * group)
        outbox[p, :group, :] = picked[rows, :]
        outbox[p, group : group + 1, :] = column_to_row(top[rows, :])
        outbox[p, group + 1 : group + 2, :] = column_to_row(total[rows, :])
        outbox[p, group + 2 :, :] = jnp.zeros((STAT_ROWS - 2, LANES), jnp.float32)
    for j in range(1, n_b):
        to = (b + j) % n_b
        sent.append(send(outbox.at[to], inbox.at[b], t_send.at[j], t_recv.at[b], (v, to)))
    parts = [outbox[b]]
    for j in range(1, n_b):
        source = (b - j + n_b) % n_b
        pltpu.make_async_copy(outbox.at[0], inbox.at[source], t_recv.at[source]).wait()
        parts.append(inbox[source])
    candidates, top, total = combine(parts, group)
    midbox[:group, :] = candidates
    midbox[group : group + 1, :] = top
    midbox[group + 1 : group + 2, :] = total
    midbox[group + 2 :, :] = jnp.zeros((STAT_ROWS - 2, LANES), jnp.float32)
    for j in range(1, n_v):
        to = (v + j) % n_v
        sent.append(send(midbox, lastbox.at[v], u_send.at[j], u_recv.at[v], (to, b)))
    lastbox[v] = midbox[...]
    for j in range(1, n_v):
        source = (v - j + n_v) % n_v
        pltpu.make_async_copy(midbox, lastbox.at[source], u_recv.at[source]).wait()
    candidates, top, total = combine([lastbox[s] for s in range(n_v)], group)

    log_norm = top + jnp.log(jnp.where(total > 0.0, total, 1.0))
    cutoff = row_to_column(keep_ref[...].astype(jnp.float32), b * group, group)
    kept = iota((group, LANES), 1).astype(jnp.float32) < cutoff
    kept_top = jnp.max(jnp.where(kept, candidates, -3e38), axis=1, keepdims=True)
    shifted = jnp.where(kept, candidates - kept_top, 0.0)
    kept_exp = jnp.where(kept, jnp.exp(shifted), 0.0)
    kept_sum = jnp.sum(kept_exp, axis=1, keepdims=True)
    kept_log = column_to_row(kept_top + jnp.log(kept_sum))
    norm_ref[...] = log_norm[:, :group]
    mass_ref[...] = (kept_log - log_norm)[:, :group]
    renorm_ref[...] = kept_exp / kept_sum
    for copy in sent:
        copy.wait_send()


def solution(mesh):
    n_v, n_b = mesh.shape["vocab"], mesh.shape["batch"]

    def local(rows, gain, w, heat, choice, ids, keep):
        group, fpd = rows.shape
        depth, cols = w.shape
        slots = n_b * group
        kc = min(fpd, CHUNK_ROWS)
        n_slots = min(depth // kc, max(1, STREAM_BYTES // (kc * cols * 2)))
        box = group + STAT_ROWS
        vmem = pl.BlockSpec(memory_space=pltpu.VMEM)
        log_norm, mass, renormed = pl.pallas_call(
            functools.partial(kernel, n_v, n_b, n_slots, kc),
            out_shape=(
                jax.ShapeDtypeStruct((1, group), jnp.float32),
                jax.ShapeDtypeStruct((1, group), jnp.float32),
                jax.ShapeDtypeStruct((group, ids.shape[1]), jnp.float32),
            ),
            in_specs=[vmem, vmem, pl.BlockSpec(memory_space=pl.ANY), vmem, vmem, vmem, vmem],
            out_specs=(vmem, vmem, vmem),
            scratch_shapes=[
                pltpu.VMEM((n_slots, kc, cols), jnp.bfloat16),
                pltpu.VMEM((n_b, n_v, group, fpd), jnp.bfloat16),
                pltpu.VMEM((depth // kc, slots, kc), jnp.bfloat16),
                pltpu.VMEM((slots, cols), jnp.float32),
                pltpu.VMEM((n_b, box, LANES), jnp.float32),
                pltpu.VMEM((n_b, box, LANES), jnp.float32),
                pltpu.VMEM((box, LANES), jnp.float32),
                pltpu.VMEM((n_v, box, LANES), jnp.float32),
                pltpu.SemaphoreType.DMA((n_slots,)),
                pltpu.SemaphoreType.DMA((n_b, n_v)),
                pltpu.SemaphoreType.DMA((n_v,)),
                pltpu.SemaphoreType.DMA((n_b // 2, n_v)),
                pltpu.SemaphoreType.DMA((n_b // 2, n_v)),
                pltpu.SemaphoreType.DMA((n_b,)),
                pltpu.SemaphoreType.DMA((n_b,)),
                pltpu.SemaphoreType.DMA((n_v,)),
                pltpu.SemaphoreType.DMA((n_v,)),
            ],
            compiler_params=pltpu.CompilerParams(
                collective_id=0,
                has_side_effects=True,
                vmem_limit_bytes=60 * 1024 * 1024,
            ),
        )(
            rows,
            gain.astype(jnp.float32).reshape(n_v, fpd),
            w,
            heat.reshape(1, -1),
            choice.reshape(1, -1),
            ids,
            keep.reshape(1, -1),
        )
        return log_norm.reshape(group), mass.reshape(group), renormed

    placed = (P("batch", "vocab"), P(), P(None, ("vocab", "batch")), P(), P(), P(), P())
    return jax.shard_map(
        local,
        mesh=mesh,
        in_specs=placed,
        out_specs=(P("batch"), P("batch"), P("batch", None)),
        check_vma=False,
    )
```
